32 devices in a mesh: seq: 8 (over z, y), tp: 4 (over x, core).
Axes of the slice: x: 2, y: 2, z: 4, core: 2. Of those that a mesh axis runs over, the one named last changes fastest.
Arguments:
- inputs: bfloat16 [2, 32, 8192], P(None, 'seq', 'tp'), may hold values from -6 to 6
- out_grad: bfloat16 [2, 32, 8192], P(None, 'seq', 'tp'), may hold values from -6 to 6
- gate_weight: bfloat16 [8192, 14848], P('tp', 'seq'), may hold values from -0.0625 to 0.0625
- up_weight: bfloat16 [8192, 14848], P('tp', 'seq'), may hold values from -0.0625 to 0.0625
- down_weight: bfloat16 [14848, 8192], P('seq', 'tp'), may hold values from -0.0625 to 0.0625
Outputs:
- input_grad: bfloat16 [2, 32, 8192], P(None, 'seq', 'tp')
- gate_grad: float32 [8192, 14848], P('tp', 'seq')
- up_grad: float32 [8192, 14848], P('tp', 'seq')
- down_grad: float32 [14848, 8192], P('seq', 'tp')
The draws below stay inside these ranges and needn't reach their ends.
All inputs are finite; a program needn't handle non-finite values.
Results may differ from the reference program's by a relative error of at most 0.0049.
Values may be sent and summed in bfloat16 or wider, within the bound.
No kernel may reach another device: no remote copies, remote signals or barrier semaphores. Data moves between devices by JAX's collectives and lax.ppermute only.
A program may use at most 128 MiB of HBM per device.

```python
import jax
import jax.numpy as jnp

D = 8192
FFW = 14848
GROUPS = 2
TC = 32


def steps_of(rng, shape, pieces, least, high):
    factor_of = 1.0
    for axis_at, shards_of in pieces:
        draws = jax.random.uniform(jax.random.fold_in(jax.random.fold_in(rng, 6), axis_at), (shards_of,), jnp.float32, least / len(pieces), high / len(pieces))
        factor_of = factor_of * jnp.repeat(jnp.exp(draws), shape[axis_at] // shards_of).reshape((-1,) + (1,) * (len(shape) - 1 - axis_at))
    return factor_of


def normal_values(own_key, dims, scale, bound, shards=(), kind=jnp.bfloat16):
    array = jax.random.normal(own_key, dims, jnp.float32) * scale
    if len(shards) > 0:
        array = steps_of(own_key, dims, shards, -0.22, 0.18) * array
    return jnp.clip(array, min=-bound, max=bound).astype(kind)


def setup_inputs(seed: int = 0) -> dict:
    key_of = jax.random.split(jax.random.key(seed), 6)
    return {
        "inputs": normal_values(key_of[0], (GROUPS, TC, D), 1.0, 6.0, ((1, 8), (2, 4))),
        "out_grad": normal_values(key_of[1], (GROUPS, TC, D), 1.0, 6.0, ((1, 8), (2, 4))),
        "gate_weight": normal_values(key_of[2], (D, FFW), D ** -0.5, 0.0625, ((0, 4), (1, 8))),
        "up_weight": normal_values(key_of[3], (D, FFW), D ** -0.5, 0.0625, ((0, 4), (1, 8))),
        "down_weight": normal_values(key_of[4], (FFW, D), D ** -0.5, 0.0625, ((0, 8), (1, 4))),
    }


def reference(inputs, out_grad, gate_weight, up_weight, down_weight):
    gate_total = jnp.zeros((D, FFW), jnp.float32)
    up_total = jnp.zeros((D, FFW), jnp.float32)
    down_total = jnp.zeros((FFW, D), jnp.float32)
    results = []
    for index in range(GROUPS):
        block_in = inputs[index]
        block_grad = out_grad[index]
        gate = jnp.dot(block_in, gate_weight, preferred_element_type=jnp.float32)
        up_proj = jnp.dot(block_in, up_weight, preferred_element_type=jnp.float32)
        hidden = (jax.nn.silu(gate) * up_proj).astype(jnp.bfloat16)
        hidden_grad = jnp.dot(block_grad, down_weight.T, preferred_element_type=jnp.float32)
        sig = jax.nn.sigmoid(gate)
        up_unit = (hidden_grad * gate * sig).astype(jnp.bfloat16)
        gate_unit = (hidden_grad * up_proj * sig * (1.0 + gate * (1.0 - sig))).astype(jnp.bfloat16)
        grad_in = jnp.dot(gate_unit, gate_weight.T, preferred_element_type=jnp.float32)
        grad_in = grad_in + jnp.dot(up_unit, up_weight.T, preferred_element_type=jnp.float32)
        results.append(grad_in.astype(jnp.bfloat16))
        gate_total = gate_total + jnp.dot(block_in.T, gate_unit, preferred_element_type=jnp.float32)
        up_total = up_total + jnp.dot(block_in.T, up_unit, preferred_element_type=jnp.float32)
        down_total = down_total + jnp.dot(hidden.T, block_grad, preferred_element_type=jnp.float32)
    return jnp.stack(results), gate_total, up_total, down_total
```

```python
import jax
import jax.numpy as jnp
from jax import lax
from jax.sharding import PartitionSpec as P

CONTRACT_FIRST = (((0,), (0,)), ((), ()))
CONTRACT_LAST = (((1,), (1,)), ((), ()))


def swap(value, axis, bit):
    count = lax.axis_size(axis)
    return lax.ppermute(value, axis, [(index, index ^ bit) for index in range(count)])


def bits_of(count):
    return [1 << power for power in reversed(range(count.bit_length() - 1))]


def dot(left, right, dims):
    return lax.dot_general(left, right, dims, preferred_element_type=jnp.float32)


def per_device(inputs, out_grad, gate_weight, up_weight, down_weight):
    blocks, local_rows, width = inputs.shape
    seq_bits = bits_of(lax.axis_size("seq"))
    tp_bits = bits_of(lax.axis_size("tp"))
    odd = (lax.axis_index("tp") & 1) == 1

    def gather(value):
        value = value.reshape(blocks * local_rows, width)
        for bit in seq_bits[:-1]:
            value = jnp.concatenate([value, swap(value, "seq", bit)])
        other = swap(value, "seq", seq_bits[-1])
        return jnp.concatenate([jnp.where(odd, other, value), jnp.where(odd, value, other)])

    def reduce(part):
        half = part.shape[0] // 2
        total = part[:half] + swap(part[half:], "tp", 1)
        for bit in tp_bits[:-1]:
            total = total + swap(total.astype(jnp.bfloat16), "tp", bit).astype(jnp.float32)
        return total

    def spread(value):
        return jnp.concatenate([value, swap(value, "tp", 1)])

    whole_in = gather(inputs)
    whole_grad = gather(out_grad)
    gate = reduce(jnp.dot(whole_in, gate_weight, preferred_element_type=jnp.float32))
    up_proj = reduce(jnp.dot(whole_in, up_weight, preferred_element_type=jnp.float32))
    hidden_grad = reduce(dot(whole_grad, down_weight, CONTRACT_LAST))
    sig = jax.nn.sigmoid(gate)
    hidden = spread((gate * sig * up_proj).astype(jnp.bfloat16))
    up_unit = spread((hidden_grad * gate * sig).astype(jnp.bfloat16))
    gate_unit = spread(
        (hidden_grad * up_proj * sig * (1.0 + gate * (1.0 - sig))).astype(jnp.bfloat16)
    )
    back = dot(gate_unit, gate_weight, CONTRACT_LAST) + dot(up_unit, up_weight, CONTRACT_LAST)
    half = back.shape[0] // 2
    sent = jnp.where(odd, back[:half], back[half:])
    kept = jnp.where(odd, back[half:], back[:half])
    back = kept + swap(sent, "seq", seq_bits[-1])
    for bit in reversed(seq_bits[:-1]):
        half = back.shape[0] // 2
        back = back[:half] + swap(back[half:], "seq", bit)
    input_grad = back.astype(jnp.bfloat16).reshape(blocks, local_rows, width)
    down_grad = dot(hidden, whole_grad, CONTRACT_FIRST)
    gate_grad = dot(whole_in, gate_unit, CONTRACT_FIRST)
    up_grad = dot(whole_in, up_unit, CONTRACT_FIRST)
    return input_grad, gate_grad, up_grad, down_grad


def solution(mesh):
    return jax.shard_map(
        per_device,
        mesh=mesh,
        in_specs=(
            P(None, "seq", "tp"),
            P(None, "seq", "tp"),
            P("tp", "seq"),
            P("tp", "seq"),
            P("seq", "tp"),
        ),
        out_specs=(P(None, "seq", "tp"), P("tp", "seq"), P("tp", "seq"), P("seq", "tp")),
        check_vma=False,
    )
```

```python
import jax
import jax.numpy as jnp
from jax import lax
from jax.experimental import pallas as pl
from jax.experimental.pallas import tpu as pltpu
from jax.sharding import PartitionSpec as P

CONTRACT_FIRST = (((0,), (0,)), ((), ()))
CONTRACT_MIDDLE = (((1,), (0,)), ((), ()))
CONTRACT_LAST = (((1,), (1,)), ((), ()))
TILE = 128
SLOTS = 8
LIMIT = 12 << 20
DIRECT = 2
STACKED = 2
STACK_FLOPS = 1 << 32
STACK_BYTES = 1 << 24


def swap(value, axis, bit):
    count = lax.axis_size(axis)
    return lax.ppermute(value, axis, [(index, index ^ bit) for index in range(count)])


def bits_of(count):
    return [1 << power for power in reversed(range(count.bit_length() - 1))]


def dot(left, right, dims):
    return lax.dot_general(left, right, dims, preferred_element_type=jnp.float32)


def outer_kernel(low_ref, high_ref, near_ref, far_ref, out_ref, left, right, held, sems):
    height = out_ref.shape[0]
    half = low_ref.shape[0]
    left[:half] = low_ref[...]
    left[half:] = high_ref[...]
    right[:half] = near_ref[...]
    right[half:] = far_ref[...]
    copies = []
    for step, start in enumerate(reversed(range(0, height, TILE))):
        rows = min(TILE, height - start)
        slot = step % SLOTS
        if step >= SLOTS:
            copies[step - SLOTS].wait()
        held[slot, :rows] = dot(left[:, start : start + rows], right[...], CONTRACT_FIRST)
        copy = pltpu.make_async_copy(
            held.at[slot, pl.ds(0, rows)], out_ref.at[pl.ds(start, rows)], sems.at[slot]
        )
        copy.start()
        copies.append(copy)
    for copy in copies[-SLOTS:]:
        copy.wait()


def outer(lefts, rights):
    half, height = lefts[0].shape
    width = rights[0].shape[1]
    rows = 2 * half
    return pl.pallas_call(
        outer_kernel,
        in_specs=[pl.BlockSpec(memory_space=pltpu.VMEM)] * 4,
        out_specs=pl.BlockSpec(memory_space=pl.ANY),
        out_shape=jax.ShapeDtypeStruct((height, width), jnp.float32),
        scratch_shapes=[
            pltpu.VMEM((rows, height), jnp.bfloat16),
            pltpu.VMEM((rows, width), jnp.bfloat16),
            pltpu.VMEM((SLOTS, TILE, width), jnp.float32),
            pltpu.SemaphoreType.DMA((SLOTS,)),
        ],
        compiler_params=pltpu.CompilerParams(vmem_limit_bytes=LIMIT),
        cost_estimate=pl.CostEstimate(
            flops=2 * rows * height * width,
            bytes_accessed=4 * height * width,
            transcendentals=0,
        ),
    )(*lefts, *rights)


def stack_kernel(low_ref, high_ref, out_ref):
    half = low_ref.shape[0]
    out_ref[:half] = low_ref[...]
    out_ref[half:] = high_ref[...]


def stack(low, high):
    return pl.pallas_call(
        stack_kernel,
        in_specs=[pl.BlockSpec(memory_space=pltpu.VMEM)] * 2,
        out_specs=pl.BlockSpec(memory_space=pltpu.VMEM),
        out_shape=jax.ShapeDtypeStruct((2 * low.shape[0], low.shape[1]), low.dtype),
        compiler_params=pltpu.CompilerParams(vmem_limit_bytes=2 << 20),
        cost_estimate=pl.CostEstimate(
            flops=STACK_FLOPS, bytes_accessed=STACK_BYTES, transcendentals=0
        ),
    )(low, high)


def layer(inputs, out_grad, gate_weight, up_weight, down_weight):
    blocks, local_rows, width = inputs.shape
    share = blocks * local_rows
    seq_bits = bits_of(lax.axis_size("seq"))
    tp_bits = bits_of(lax.axis_size("tp"))
    odd = (lax.axis_index("tp") & 1) == 1

    def gather(value):
        for index, bit in enumerate(seq_bits[:-1]):
            other = swap(value, "seq", bit)
            if value.ndim == 3:
                value = value.reshape(share, width)
                other = other.reshape(share, width)
            if index < STACKED:
                value = stack(value, other)
            else:
                value = jnp.concatenate([value, other])
        return value, swap(value, "seq", 1)

    def turn(own, other):
        return jnp.where(odd, other, own), jnp.where(odd, own, other)

    def reduce(kept, sent):
        total = kept + swap(sent, "tp", 1)
        for bit in tp_bits[:-1]:
            other = swap(total.astype(jnp.bfloat16), "tp", bit)
            total = total + other.astype(jnp.float32)
        return total

    def spread(value):
        return value, swap(value, "tp", 1)

    def halves(part):
        half = part.shape[0] // 2
        return part[:half], part[half:]

    near_in = lax.optimization_barrier(turn(*gather(inputs)))
    gate_part = dot(jnp.concatenate(near_in), gate_weight, CONTRACT_MIDDLE)
    near_grad, gate_part = lax.optimization_barrier((gather(out_grad), gate_part))
    near_grad = turn(*near_grad)
    up_part = dot(jnp.concatenate(near_in), up_weight, CONTRACT_MIDDLE)
    near_grad, up_part = lax.optimization_barrier((near_grad, up_part))
    hidden_grad_part = dot(jnp.concatenate(near_grad), down_weight, CONTRACT_LAST)
    gate = reduce(*halves(gate_part))
    up_proj = reduce(*halves(up_part))
    hidden = (gate * jax.nn.sigmoid(gate) * up_proj).astype(jnp.bfloat16)
    hidden = spread(hidden)
    down_grad = outer(hidden, near_grad)
    hidden_grad = reduce(*halves(hidden_grad_part))
    hidden, gate, up_proj, hidden_grad = lax.optimization_barrier(
        (hidden, gate, up_proj, hidden_grad)
    )
    sig = jax.nn.sigmoid(gate)
    up_unit = spread((hidden_grad * gate * sig).astype(jnp.bfloat16))
    gate_unit = spread(
        (hidden_grad * up_proj * sig * (1.0 + gate * (1.0 - sig))).astype(jnp.bfloat16),
    )
    back = dot(jnp.concatenate(gate_unit), gate_weight, CONTRACT_LAST)
    back = back + dot(jnp.concatenate(up_unit), up_weight, CONTRACT_LAST)
    half = back.shape[0] // 2
    sent = jnp.where(odd, back[:half], back[half:])
    kept = jnp.where(odd, back[half:], back[:half])
    back = kept + swap(sent.astype(jnp.bfloat16), "seq", 1).astype(jnp.float32)
    for place in reversed(range(DIRECT, len(seq_bits) - 1)):
        half = back.shape[0] // 2
        back = back[:half] + swap(back[half:], "seq", seq_bits[place])
    total = back[:share]
    for index in range(1, back.shape[0] // share):
        bits = [bit for place, bit in enumerate(seq_bits[:-1]) if index >> place & 1]
        block = back[index * share : (index + 1) * share]
        total = total + swap(block, "seq", sum(bits))
    input_grad = total.astype(jnp.bfloat16).reshape(blocks, local_rows, width)
    gate_grad = outer(gate_unit, near_in).T
    up_grad = outer(up_unit, near_in).T
    return input_grad, gate_grad, up_grad, down_grad


def solution(mesh):
    return jax.shard_map(
        layer,
        mesh=mesh,
        in_specs=(
            P(None, "seq", "tp"),
            P(None, "seq", "tp"),
            P("tp", "seq"),
            P("tp", "seq"),
            P("seq", "tp"),
        ),
        out_specs=(P(None, "seq", "tp"), P("tp", "seq"), P("tp", "seq"), P("seq", "tp")),
        check_vma=False,
    )
```
